32 devices in a mesh: rel: 4 (over z), node: 2 (over x), head: 4 (over y, core).
Axes of the slice: x: 2, y: 2, z: 4, core: 2. Of those that a mesh axis runs over, the one named last changes fastest.
Arguments:
- features: bfloat16 [4096, 512], P('node'), may hold values from -26 to 26
- node_type: int32 [4096], P('node'), may hold values from 0 to 3
- w_query: bfloat16 [4, 512, 512], P(None, None, 'head'), may hold values from -0.25 to 0.25
- w_key: bfloat16 [4, 512, 512], P(None, None, 'head'), may hold values from -0.25 to 0.25
- w_value: bfloat16 [4, 512, 512], P(None, None, 'head'), may hold values from -0.25 to 0.25
- rel_att: bfloat16 [64, 8, 64, 64], P(None, 'head'), may hold values from -0.75 to 0.75
- rel_msg: bfloat16 [64, 8, 64, 64], P(None, 'head'), may hold values from -0.75 to 0.75
- rel_prior: float32 [64, 8], P(None, 'head'), may hold values from 0.5 to 3
- w_out: bfloat16 [4, 512, 512], P(None, 'head'), may hold values from -0.25 to 0.25
- skip: float32 [4], replicated, may hold values from -1.5 to 1.5
- rel_perm: int32 [64], P('rel'), may hold values from 0 to 63, each once
- tile_src: int32 [64, 32], P('rel', 'node'), may hold values from 0 to 31
- tile_dst: int32 [64, 32], P('rel', 'node'), may hold values from 0 to 15
- tile_bits: int32 [64, 32, 128, 4], P('rel', 'node'), may hold values from -2147483648 to 2147483646
- tile_count: int32 [64, 2], P('rel', 'node'), may hold values from 1 to 16, as said below
Outputs:
- updated: bfloat16 [4096, 512], P(('node', 'head'))
The draws below stay inside these ranges and needn't reach their ends.
Inputs may be any that keep to these rules, and one draw needn't show every extreme that they name: The first tile_count[p, g] slots of group g of position p are live; the words of the other slots may have bits set, but those bits give no edges and must be ignored. Some position has all 16 slots live in every group.
All inputs are finite; a program needn't handle non-finite values.
Results may differ from the reference program's by a relative error of at most 0.008.
The reference program's roundings to bfloat16 on the way (of `qrel` and `hidden`) count: a program that leaves them out, or rounds other values in their place, can miss the bound.
Values may be sent and summed in bfloat16 or wider, within the bound.
A program may use at most 128 MiB of HBM per device.

```python
import math
import jax
import jax.numpy as jnp
from jax import lax

D = 512
HEADS = 8
TYPES = 4
RELS = 64
BLOCK = 128
NB_DEV = 16
TCAP = 16
HD = 64
WORDS = 4
NSHARD = 2
NBLOCKS = 32
NODES = 4096
TILE_SLOTS = 32


def draw_features(key, part):
    first = jax.random.fold_in(key, 0)
    base = jnp.clip(jax.random.normal(first, (NODES, D), jnp.float32), -6.0, 6.0)
    return base.astype(jnp.bfloat16)


def draw_tile_count(key, part):
    first, second, third = jax.random.split(key, 3)
    lowest = max(TCAP // 10, 1)
    sizes = jax.random.randint(first, (RELS, 1), lowest, TCAP + 1)
    drops = jax.random.randint(second, (RELS, NSHARD), 0, 4)
    counts = sizes - drops * sizes // 8
    chosen = jax.random.randint(third, (), 0, RELS)
    rows = jnp.arange(RELS, dtype=jnp.int32)[:, None]
    counts = jnp.where(rows == chosen, TCAP, counts)
    return jnp.maximum(counts, 1).astype(jnp.int32)


def slot_targets(key):
    return jax.random.randint(jax.random.fold_in(key, 11), (RELS, TILE_SLOTS), 0, NB_DEV).astype(jnp.int32)


def draw_tile_dst(key, part):
    return slot_targets(key)


def draw_tile_bits(key, part):
    targets = slot_targets(key)
    packed = jax.random.randint(jax.random.fold_in(key, 13), (RELS, TILE_SLOTS, BLOCK, WORDS), -2147483648, 2147483647, dtype=jnp.int32)
    marked = jax.random.randint(jax.random.fold_in(key, 17), (NBLOCKS, BLOCK), 0, 16)
    chosen = jax.random.randint(jax.random.fold_in(key, 19), (), 0, NBLOCKS * BLOCK)
    node_ids = jnp.arange(NBLOCKS * BLOCK, dtype=jnp.int32).reshape(NBLOCKS, BLOCK)
    lonely = (marked == 0) | (node_ids == chosen)
    groups = jnp.arange(TILE_SLOTS, dtype=jnp.int32) // TCAP
    blocks = (groups[None, :] * NB_DEV + targets).astype(jnp.int32)
    silenced = lonely[blocks]
    return jnp.where(silenced[..., None], 0, packed).astype(jnp.int32)


def with_ends(result, own_key, smallest, top_value):
    longest = result.shape.index(max(result.shape))
    spots = []
    for shift in (0, 1):
        where = [jax.random.randint(jax.random.fold_in(own_key, axis), (), 0, length) for axis, length in enumerate(result.shape)]
        where[longest] = (where[longest] + shift) % result.shape[longest]
        spots.append(tuple(where))
    return result.at[spots[0]].set(smallest).at[spots[1]].set(top_value)


def steps_of(rng, shape, pieces, low, largest):
    level, own = 1.0, jax.random.fold_in(rng, 6)
    for position, shards_of in pieces:
        draws = jnp.exp(jax.random.uniform(jax.random.fold_in(own, position), (shards_of,), jnp.float32, low / len(pieces), largest / len(pieces)))
        level = level * jnp.repeat(draws, shape[position] // shards_of).reshape([-1 if axis == position else 1 for axis in range(len(shape))])
    return level


def normal_values(stream_key, shape, spread, bound, cuts=(), held_as=jnp.bfloat16):
    factor_of = steps_of(stream_key, shape, cuts, -0.22, 0.18) if cuts else 1.0
    array = jax.random.normal(stream_key, shape, jnp.float32) * spread * factor_of
    return jnp.minimum(jnp.maximum(array, -bound), bound).astype(held_as)


def setup_inputs(seed: int = 0) -> dict:
    seeds = jax.random.split(jax.random.key(seed), 16)
    return {
        "features": draw_features(jax.random.fold_in(seeds[15], 71), 0),
        "node_type": with_ends(jax.random.randint(seeds[1], (NODES,), 0, TYPES), jax.random.fold_in(seeds[1], 1), 0, TYPES - 1).astype(jnp.int32),
        "w_query": normal_values(seeds[2], (TYPES, D, D), D ** -0.5, 0.25, ((2, 4),)),
        "w_key": normal_values(seeds[3], (TYPES, D, D), D ** -0.5, 0.25, ((2, 4),)),
        "w_value": normal_values(seeds[4], (TYPES, D, D), D ** -0.5, 0.25, ((2, 4),)),
        "rel_att": normal_values(seeds[5], (RELS, HEADS, HD, HD), HD ** -0.5, 0.75, ((1, 4),)),
        "rel_msg": normal_values(seeds[6], (RELS, HEADS, HD, HD), HD ** -0.5, 0.75, ((1, 4),)),
        "rel_prior": jnp.clip(jnp.exp(math.log(3.0) - 1.7917595 * jax.random.uniform(seeds[7], (RELS, HEADS), jnp.float32) ** steps_of(seeds[7], (RELS, HEADS), ((1, 4),), -0.2, 0.2)), 0.5, 3.0),
        "w_out": normal_values(seeds[8], (TYPES, D, D), D ** -0.5, 0.25, ((1, 4),)),
        "skip": jnp.clip(jax.random.uniform(seeds[9], (TYPES,), jnp.float32, -1.5, 1.5), -1.5, 1.5),
        "rel_perm": jax.random.permutation(seeds[10], RELS).astype(jnp.int32),
        "tile_src": with_ends(jax.random.randint(seeds[11], (RELS, TILE_SLOTS), 0, NBLOCKS), jax.random.fold_in(seeds[11], 1), 0, NBLOCKS - 1).astype(jnp.int32),
        "tile_dst": draw_tile_dst(jax.random.fold_in(seeds[15], 71), 0),
        "tile_bits": draw_tile_bits(jax.random.fold_in(seeds[15], 71), 0),
        "tile_count": draw_tile_count(jax.random.fold_in(seeds[15], 71), 0),
    }


NEG = -1e+30

def project(rows, types, weights):
    total = jnp.zeros((rows.shape[0], weights.shape[2]), jnp.float32)
    for kind in range(weights.shape[0]):
        partial_out = jnp.dot(rows, weights[kind], preferred_element_type=jnp.float32)
        total = jnp.where((types == kind)[:, None], partial_out, total)
    return total

def unpack(words):
    shifts = jnp.arange(32, dtype=jnp.int32)
    bits = words[..., None] >> shifts & 1
    return bits.reshape(words.shape[:-1] + (words.shape[-1] * 32,)) > 0

def reference(features, node_type, w_query, w_key, w_value, rel_att, rel_msg, rel_prior, w_out, skip, rel_perm, tile_src, tile_dst, tile_bits, tile_count):
    query = project(features, node_type, w_query).astype(jnp.bfloat16)
    key = project(features, node_type, w_key).astype(jnp.bfloat16)
    value = project(features, node_type, w_value).astype(jnp.bfloat16)
    query_f = query.reshape(NODES, HEADS, HD).astype(jnp.float32)
    key_blocks = key.reshape(NBLOCKS, BLOCK, HEADS, HD)
    value_blocks = value.reshape(NBLOCKS, BLOCK, HEADS, HD)
    factor = 1.0 / math.sqrt(HD)
    slot_ids = jnp.arange(TILE_SLOTS, dtype=jnp.int32)
    shard = slot_ids // TCAP

    def visit(carry, item):
        m_run, l_run, acc = carry
        relation, src, dst_local, words, counts = item
        live = slot_ids % TCAP < counts[shard]
        dst = (shard * NB_DEV + dst_local).astype(jnp.int32)
        att = rel_att[relation].astype(jnp.float32)
        msg_w = rel_msg[relation].astype(jnp.float32)
        prior = rel_prior[relation] * factor
        qrel = (jnp.einsum('nhe,hde->nhd', query_f, att) * prior[None, :, None]).astype(jnp.bfloat16)
        qrel = qrel.reshape(NBLOCKS, BLOCK, HEADS, HD)
        q_t = qrel[dst].astype(jnp.float32)
        k_t = key_blocks[src].astype(jnp.float32)
        v_t = value_blocks[src].astype(jnp.float32)
        message = jnp.einsum('sjhd,hde->sjhe', v_t, msg_w).astype(jnp.bfloat16)
        scores = jnp.einsum('sihd,sjhd->shij', q_t, k_t)
        edges = unpack(words) & live[:, None, None]
        masked = jnp.where(edges[:, None], scores, NEG)
        block_top = jax.ops.segment_max(masked.max(-1), dst, num_segments=NBLOCKS)
        m_new = jnp.maximum(m_run, block_top)
        weights = jnp.where(edges[:, None], jnp.exp(masked - m_new[dst][..., None]), 0.0)
        rescale = jnp.exp(m_run - m_new)
        l_new = l_run * rescale + jax.ops.segment_sum(weights.sum(-1), dst, num_segments=NBLOCKS)
        pv = jnp.einsum('shij,sjhe->sihe', weights.astype(jnp.bfloat16).astype(jnp.float32), message.astype(jnp.float32))
        acc_new = acc * rescale.transpose(0, 2, 1)[..., None] + jax.ops.segment_sum(pv, dst, num_segments=NBLOCKS)
        return ((m_new, l_new, acc_new), None)
    init = (jnp.full((NBLOCKS, HEADS, BLOCK), NEG, jnp.float32), jnp.zeros((NBLOCKS, HEADS, BLOCK), jnp.float32), jnp.zeros((NBLOCKS, BLOCK, HEADS, HD), jnp.float32))
    (m_run, l_run, acc), _ = lax.scan(visit, init, (rel_perm, tile_src, tile_dst, tile_bits, tile_count))
    totals = l_run.transpose(0, 2, 1).reshape(NODES, HEADS)
    agg = acc.reshape(NODES, D) / jnp.repeat(jnp.maximum(totals, 1.0), HD, axis=1)
    hidden = jax.nn.gelu(agg).astype(jnp.bfloat16)
    mixed = project(hidden, node_type, w_out)
    gate = jax.nn.sigmoid(skip)[node_type][:, None]
    return (gate * mixed + (1.0 - gate) * features.astype(jnp.float32)).astype(jnp.bfloat16)
```

```python
import functools
import math

import jax
import jax.numpy as jnp
from jax import lax
from jax.experimental import pallas as pl
from jax.experimental.pallas import tpu as pltpu
from jax.sharding import PartitionSpec as P

NEG = -1e30
FLOOR = -1e29
UNROLL = 4
VMEM_BYTES = 56 * 1024 * 1024


def project(rows, types, weights):
    total = jnp.zeros((rows.shape[0], weights.shape[2]), jnp.float32)
    for kind in range(weights.shape[0]):
        partial_out = jnp.dot(rows, weights[kind], preferred_element_type=jnp.float32)
        total = jnp.where((types == kind)[:, None], partial_out, total)
    return total


def gate_of(kinds, skip):
    table = jax.nn.sigmoid(skip)
    hits = kinds[:, None] == jnp.arange(skip.shape[0], dtype=jnp.int32)[None, :]
    return jnp.sum(jnp.where(hits, table[None, :], 0.0), axis=1)[:, None]


def column(types_row):
    size = types_row.shape[1]
    return jnp.broadcast_to(types_row.astype(jnp.float32), (size, size)).T


def kv_kernel(x_ref, types_ref, wk_ref, wv_ref, k_ref, vt_ref):
    per, block, cols = k_ref.shape
    kinds = wk_ref.shape[0]
    x = x_ref[...]
    masks = [column(types_ref[0, b : b + 1, :]) for b in range(per)]
    totals = [None] * per
    for kind in range(kinds):
        both = jnp.concatenate([wk_ref[kind], wv_ref[kind]], axis=1)
        out = jnp.dot(x, both, preferred_element_type=jnp.float32)
        for b in range(per):
            piece = out[b * block : (b + 1) * block]
            pair = (piece[:, :cols], piece[:, cols:])
            if totals[b] is None:
                totals[b] = pair
            else:
                hit = masks[b] == float(kind)
                totals[b] = tuple(jnp.where(hit, n, o) for n, o in zip(pair, totals[b]))
    for b in range(per):
        k_ref[b] = totals[b][0].astype(jnp.bfloat16)
        vt_ref[b] = totals[b][1].T.astype(jnp.bfloat16)


def q_kernel(per_pos, perm_ref, x_ref, types_ref, wq_ref, *refs):
    att_refs, msg_refs = refs[:per_pos], refs[per_pos : 2 * per_pos]
    qt_ref, att_out, msg_out = refs[2 * per_pos :]
    per, block, cols = qt_ref.shape[0], qt_ref.shape[2], qt_ref.shape[1]
    kinds = wq_ref.shape[0]
    x = x_ref[...]
    wide = jnp.concatenate([wq_ref[kind] for kind in range(kinds)], axis=1)
    out = jnp.dot(x, wide, preferred_element_type=jnp.float32)
    for b in range(per):
        mask = column(types_ref[0, b : b + 1, :])
        piece = out[b * block : (b + 1) * block]
        total = piece[:, :cols]
        for kind in range(1, kinds):
            total = jnp.where(mask == float(kind), piece[:, kind * cols : (kind + 1) * cols], total)
        qt_ref[b] = total.T.astype(jnp.bfloat16)

    def diagonal(ref):
        heads, size = ref.shape[1], ref.shape[2]
        rows = []
        for h in range(heads):
            parts = [jnp.zeros((size, size), jnp.float32)] * heads
            parts[h] = ref[0, h].astype(jnp.float32)
            rows.append(jnp.concatenate(parts, axis=1))
        return jnp.concatenate(rows, axis=0)

    for i in range(per_pos):
        att_out[i] = diagonal(att_refs[i]).astype(jnp.bfloat16)
        msg_out[i] = diagonal(msg_refs[i]).T.astype(jnp.bfloat16)


def tile_kernel(
    first,
    n_node,
    heads,
    factor,
    count_ref,
    src_ref,
    dst_ref,
    perm_ref,
    prior_ref,
    qt_ref,
    k_ref,
    vt_ref,
    bits_ref,
    att_ref,
    msg_ref,
    *refs,
):
    if first:
        ml_ref, acc_ref, list_ref = refs
    else:
        ml_in, acc_in, ml_ref, acc_ref, list_ref = refs
    positions = count_ref.shape[0]
    slots = src_ref.shape[0]
    tcap = slots // positions
    blocks = qt_ref.shape[0]
    cols, block = qt_ref.shape[1], qt_ref.shape[2]
    size = cols // heads
    words = bits_ref.shape[1]
    me = lax.axis_index("node")

    if first:
        ml_ref[:, :heads] = jnp.full((blocks, heads, block), FLOOR, jnp.float32)
        ml_ref[:, heads:] = jnp.zeros((blocks, heads, block), jnp.float32)
        acc_ref[...] = jnp.zeros_like(acc_ref)
    else:
        ml_ref[...] = ml_in[...]
        acc_ref[...] = acc_in[...]

    def offset_of(src):
        return lax.rem(src // blocks - me + n_node, n_node)

    def gather_position(p, n):
        count = count_ref[p]
        for k in range(tcap):
            slot = p * tcap + k
            list_ref[n] = slot
            local = offset_of(src_ref[slot]) == 0
            mine = local if first else jnp.logical_not(local)
            n = n + jnp.where(jnp.logical_and(mine, k < count), 1, 0)
        return n

    total = lax.fori_loop(0, positions, gather_position, 0)
    for u in range(UNROLL):
        list_ref[total + u] = 0
    bit_of = lax.shift_left(
        jnp.int32(1), lax.broadcasted_iota(jnp.int32, (32, block), 0)
    )
    half = lax.broadcasted_iota(jnp.int32, (cols, 1), 0) // size

    def visit(turn, carry):
        state = []
        for u in range(UNROLL):
            index = turn * UNROLL + u
            slot = list_ref[index]
            valid = jnp.where(index < total, -1, 0)
            p = slot // tcap
            src = src_ref[slot]
            dst = dst_ref[slot]
            where_src = offset_of(src) * blocks + lax.rem(src, blocks)
            if not first:
                where_src = jnp.maximum(where_src - blocks, 0)
            else:
                where_src = lax.rem(src, blocks)
            rel = perm_ref[p]
            qr = jnp.dot(att_ref[p], qt_ref[dst], preferred_element_type=jnp.float32)
            zero = jnp.zeros((size, block), jnp.bfloat16)
            sides = []
            for h in range(heads):
                scaled = qr[h * size : (h + 1) * size] * (prior_ref[rel * heads + h] * factor)
                parts = [zero] * heads
                parts[h] = scaled.astype(jnp.bfloat16)
                sides.append(jnp.concatenate(parts, axis=0))
            scores = jnp.dot(
                k_ref[where_src],
                jnp.concatenate(sides, axis=1),
                preferred_element_type=jnp.float32,
            )
            message = jnp.dot(
                msg_ref[p], vt_ref[where_src], preferred_element_type=jnp.float32
            ).astype(jnp.bfloat16)
            tile_words = bits_ref[slot] & valid
            edges = jnp.concatenate(
                [(tile_words[w : w + 1] & bit_of) != 0 for w in range(words)], axis=0
            )
            tile = []
            for h in range(heads):
                masked = jnp.where(edges, scores[:, h * block : (h + 1) * block], NEG)
                top = jnp.maximum(jnp.max(masked, axis=0, keepdims=True), FLOOR)
                weights = jnp.exp(masked - top)
                sums = jnp.sum(weights, axis=0, keepdims=True)
                out = jnp.dot(
                    message[h * size : (h + 1) * size],
                    weights.astype(jnp.bfloat16),
                    preferred_element_type=jnp.float32,
                )
                tile.append((top, sums, out))
            state.append((dst, tile))
        for dst, tile in state:
            for h, (top, sums, out) in enumerate(tile):
                m_old = ml_ref[dst, h : h + 1]
                l_old = ml_ref[dst, heads + h : heads + h + 1]
                m_new = jnp.maximum(m_old, top)
                keep = jnp.exp(m_old - m_new)
                take = jnp.exp(top - m_new)
                ml_ref[dst, h : h + 1] = m_new
                ml_ref[dst, heads + h : heads + h + 1] = l_old * keep + sums * take
                rows = pl.ds(h * size, size)
                acc_ref[dst, rows] = acc_ref[dst, rows] * keep + out * take
        return carry

    lax.fori_loop(0, (total + UNROLL - 1) // UNROLL, visit, 0)


def per_device(
    features,
    node_type,
    w_query,
    w_key,
    w_value,
    rel_att,
    rel_msg,
    rel_prior,
    w_out,
    skip,
    rel_perm,
    tile_src,
    tile_dst,
    tile_bits,
    tile_count,
):
    node_rows, width = features.shape
    n_rel = lax.axis_size("rel")
    n_node = lax.axis_size("node")
    n_head = lax.axis_size("head")
    heads = rel_prior.shape[1]
    cols = w_query.shape[2]
    kinds = w_query.shape[0]
    head_size = cols // heads
    block = tile_bits.shape[2]
    words = tile_bits.shape[3]
    blocks = node_rows // block
    positions, tcap = tile_src.shape
    slots = positions * tcap
    factor = 1.0 / math.sqrt(head_size)
    steps = math.gcd(blocks // 2 if blocks % 2 == 0 else blocks, positions)
    per = blocks // steps
    per_pos = positions // steps
    types3 = node_type.reshape(steps, per, block)
    bf = jnp.bfloat16

    x_spec = pl.BlockSpec((per * block, width), lambda s, *_: (s, 0))
    t_spec = pl.BlockSpec((1, per, block), lambda s, *_: (s, 0, 0))
    w_spec = pl.BlockSpec((kinds, width, cols), lambda s, *_: (0, 0, 0))

    def tile_spec(count, rows, lanes):
        return pl.BlockSpec((count, rows, lanes), lambda s, *_: (s, 0, 0))

    keys, values_t = pl.pallas_call(
        kv_kernel,
        grid=(steps,),
        in_specs=[x_spec, t_spec, w_spec, w_spec],
        out_specs=[tile_spec(per, block, cols), tile_spec(per, cols, block)],
        out_shape=[
            jax.ShapeDtypeStruct((blocks, block, cols), bf),
            jax.ShapeDtypeStruct((blocks, cols, block), bf),
        ],
        name="project_kv",
    )(features, types3, w_key, w_value)

    far_k, far_v = [], []
    for shift in range(1, n_node):
        pairs = [(i, (i - shift) % n_node) for i in range(n_node)]
        far_k.append(lax.ppermute(keys, "node", pairs))
        far_v.append(lax.ppermute(values_t, "node", pairs))

    def rel_spec(i):
        return pl.BlockSpec(
            (1,) + rel_att.shape[1:], lambda s, perm: (perm[s * per_pos + i], 0, 0, 0)
        )

    rel_specs = [rel_spec(i) for i in range(per_pos)]
    query_t, att, msg = pl.pallas_call(
        functools.partial(q_kernel, per_pos),
        grid_spec=pltpu.PrefetchScalarGridSpec(
            num_scalar_prefetch=1,
            grid=(steps,),
            in_specs=[x_spec, t_spec, w_spec] + rel_specs * 2,
            out_specs=[
                tile_spec(per, cols, block),
                tile_spec(per_pos, cols, cols),
                tile_spec(per_pos, cols, cols),
            ],
        ),
        out_shape=[
            jax.ShapeDtypeStruct((blocks, cols, block), bf),
            jax.ShapeDtypeStruct((positions, cols, cols), bf),
            jax.ShapeDtypeStruct((positions, cols, cols), bf),
        ],
        name="project_q",
    )(rel_perm, features, types3, w_query, *([rel_att] * per_pos + [rel_msg] * per_pos))

    bits = tile_bits.transpose(0, 1, 3, 2).reshape(slots, words, block)
    scalars = (
        tile_count.reshape(positions),
        tile_src.reshape(slots),
        tile_dst.reshape(slots),
        rel_perm,
        rel_prior.reshape(-1),
    )
    smem = pl.BlockSpec(memory_space=pltpu.SMEM)
    vmem = pl.BlockSpec(memory_space=pltpu.VMEM)
    state = [
        jax.ShapeDtypeStruct((blocks, 2 * heads, block), jnp.float32),
        jax.ShapeDtypeStruct((blocks, cols, block), jnp.float32),
    ]

    def tiles(first, k_blocks, v_blocks, *carried):
        return pl.pallas_call(
            functools.partial(tile_kernel, first, n_node, heads, factor),
            in_specs=[smem] * 5 + [vmem] * (6 + len(carried)),
            out_specs=[vmem, vmem],
            out_shape=state,
            scratch_shapes=[pltpu.SMEM((slots + UNROLL,), jnp.int32)],
            compiler_params=pltpu.CompilerParams(vmem_limit_bytes=VMEM_BYTES),
            name="tiles_near" if first else "tiles_far",
        )(*scalars, query_t, k_blocks, v_blocks, bits, att, msg, *carried)

    ml, acc = tiles(True, keys, values_t)
    if n_node > 1:
        join = lambda arrs: arrs[0] if len(arrs) == 1 else jnp.concatenate(arrs, axis=0)
        ml, acc = tiles(False, join(far_k), join(far_v), ml, acc)

    m_rows = ml[:, :heads].transpose(0, 2, 1).reshape(node_rows, heads)
    l_rows = ml[:, heads:].transpose(0, 2, 1).reshape(node_rows, heads)
    acc_rows = acc.transpose(0, 2, 1).reshape(node_rows, cols)
    top = lax.pmax(m_rows, "rel")
    scaling = jnp.exp(m_rows - top)
    l_scaled = l_rows * scaling
    a_scaled = acc_rows * jnp.repeat(scaling, head_size, axis=1)
    piece = node_rows // (n_rel * n_head)

    def regroup(arr):
        return (
            arr.reshape(n_head, n_rel, piece, arr.shape[1])
            .transpose(1, 0, 2, 3)
            .reshape(node_rows, arr.shape[1])
        )

    a_sum, l_sum = (
        lax.psum_scatter(
            regroup(a_scaled).astype(jnp.bfloat16), "rel", scatter_dimension=0, tiled=True
        ).astype(jnp.float32),
        lax.psum_scatter(
            regroup(l_scaled).astype(jnp.bfloat16), "rel", scatter_dimension=0, tiled=True
        ).astype(jnp.float32),
    )
    kinds_grouped = node_type.reshape(n_head, n_rel, piece).transpose(1, 0, 2).reshape(node_rows)
    kinds_mine = lax.dynamic_slice_in_dim(
        kinds_grouped, lax.axis_index("rel") * n_head * piece, n_head * piece, 0
    )
    hidden = jax.nn.gelu(a_sum / jnp.repeat(jnp.maximum(l_sum, 1.0), head_size, axis=1)).astype(
        jnp.bfloat16
    )
    mixed = lax.psum_scatter(
        project(hidden, kinds_mine, w_out).astype(jnp.bfloat16),
        "head",
        scatter_dimension=0,
        tiled=True,
    ).astype(jnp.float32)
    first_row = (lax.axis_index("head") * n_rel + lax.axis_index("rel")) * piece
    resid = lax.dynamic_slice_in_dim(features, first_row, piece, 0).astype(jnp.float32)
    kinds_own = lax.dynamic_slice_in_dim(node_type, first_row, piece, 0)
    gate = gate_of(kinds_own, skip)
    finished = (gate * mixed + (1.0 - gate) * resid).astype(jnp.bfloat16)
    return lax.all_gather(finished, "rel", axis=0, tiled=True)


def solution(mesh):
    in_specs = (
        P("node", None),
        P("node"),
        P(None, None, "head"),
        P(None, None, "head"),
        P(None, None, "head"),
        P(None, "head", None, None),
        P(None, "head", None, None),
        P(None, "head"),
        P(None, "head", None),
        P(),
        P("rel"),
        P("rel", "node"),
        P("rel", "node"),
        P("rel", "node", None, None),
        P("rel", "node"),
    )
    out_specs = P(("node", "head"), None)
    return jax.shard_map(
        per_device, mesh=mesh, in_specs=in_specs, out_specs=out_specs, check_vma=False
    )
```

```python
import functools
import math

import jax
import jax.numpy as jnp
from jax import lax
from jax.experimental import pallas as pl
from jax.experimental.pallas import tpu as pltpu
from jax.sharding import PartitionSpec as P

NEG = -1e30
FLOOR = -1e29
UNROLL = 4
VMEM_BYTES = 28 * 1024 * 1024


def column(types_row):
    size = types_row.shape[1]
    return jnp.broadcast_to(types_row.astype(jnp.float32), (size, size)).T


def kv_kernel(x_ref, types_ref, wk_ref, wv_ref, k_ref, vt_ref):
    per, block, cols = k_ref.shape
    kinds = wk_ref.shape[0]
    x = x_ref[...]
    masks = [column(types_ref[0, b : b + 1, :]) for b in range(per)]
    totals = [None] * per
    for kind in range(kinds):
        both = jnp.concatenate([wk_ref[kind], wv_ref[kind]], axis=1)
        out = jnp.dot(x, both, preferred_element_type=jnp.float32)
        for b in range(per):
            piece = out[b * block : (b + 1) * block]
            pair = (piece[:, :cols], piece[:, cols:])
            if totals[b] is None:
                totals[b] = pair
            else:
                hit = masks[b] == float(kind)
                totals[b] = tuple(jnp.where(hit, n, o) for n, o in zip(pair, totals[b]))
    for b in range(per):
        k_ref[b] = totals[b][0].astype(jnp.bfloat16)
        vt_ref[b] = totals[b][1].T.astype(jnp.bfloat16)


def q_kernel(per_pos, perm_ref, x_ref, types_ref, wq_ref, *refs):
    att_refs, msg_refs = refs[:per_pos], refs[per_pos : 2 * per_pos]
    qt_ref, att_out, msg_out = refs[2 * per_pos :]
    per, block, cols = qt_ref.shape[0], qt_ref.shape[2], qt_ref.shape[1]
    kinds = wq_ref.shape[0]
    x = x_ref[...]
    wide = jnp.concatenate([wq_ref[kind] for kind in range(kinds)], axis=1)
    out = jnp.dot(x, wide, preferred_element_type=jnp.float32)
    for b in range(per):
        mask = column(types_ref[0, b : b + 1, :])
        piece = out[b * block : (b + 1) * block]
        total = piece[:, :cols]
        for kind in range(1, kinds):
            total = jnp.where(mask == float(kind), piece[:, kind * cols : (kind + 1) * cols], total)
        qt_ref[b] = total.T.astype(jnp.bfloat16)

    def diagonal(ref):
        heads, size = ref.shape[1], ref.shape[2]
        rows = []
        for h in range(heads):
            parts = [jnp.zeros((size, size), jnp.float32)] * heads
            parts[h] = ref[0, h].astype(jnp.float32)
            rows.append(jnp.concatenate(parts, axis=1))
        return jnp.concatenate(rows, axis=0)

    for i in range(per_pos):
        att_out[i] = diagonal(att_refs[i]).astype(jnp.bfloat16)
        msg_out[i] = diagonal(msg_refs[i]).T.astype(jnp.bfloat16)


def tile_kernel(
    first,
    n_node,
    heads,
    factor,
    count_ref,
    src_ref,
    dst_ref,
    perm_ref,
    prior_ref,
    qt_ref,
    k_ref,
    vt_ref,
    bits_ref,
    att_ref,
    msg_ref,
    *refs,
):
    if first:
        ml_ref, acc_ref, list_ref = refs
    else:
        ml_in, acc_in, ml_ref, acc_ref, list_ref = refs
    positions = count_ref.shape[0]
    slots = src_ref.shape[0]
    tcap = slots // positions
    blocks = qt_ref.shape[0]
    cols, block = qt_ref.shape[1], qt_ref.shape[2]
    size = cols // heads
    words = bits_ref.shape[1]
    me = lax.axis_index("node")

    if first:
        ml_ref[:, :heads] = jnp.full((blocks, heads, block), FLOOR, jnp.float32)
        ml_ref[:, heads:] = jnp.zeros((blocks, heads, block), jnp.float32)
        acc_ref[...] = jnp.zeros_like(acc_ref)
    else:
        ml_ref[...] = ml_in[...]
        acc_ref[...] = acc_in[...]

    def offset_of(src):
        return lax.rem(src // blocks - me + n_node, n_node)

    def gather_position(p, n):
        count = count_ref[p]
        for k in range(tcap):
            slot = p * tcap + k
            list_ref[n] = slot
            local = offset_of(src_ref[slot]) == 0
            mine = local if first else jnp.logical_not(local)
            n = n + jnp.where(jnp.logical_and(mine, k < count), 1, 0)
        return n

    total = lax.fori_loop(0, positions, gather_position, 0)
    for u in range(UNROLL):
        list_ref[total + u] = 0
    bit_of = lax.shift_left(
        jnp.int32(1), lax.broadcasted_iota(jnp.int32, (32, block), 0)
    )
    half = lax.broadcasted_iota(jnp.int32, (cols, 1), 0) // size

    def visit(turn, carry):
        state = []
        for u in range(UNROLL):
            index = turn * UNROLL + u
            slot = list_ref[index]
            valid = jnp.where(index < total, -1, 0)
            p = slot // tcap
            src = src_ref[slot]
            dst = dst_ref[slot]
            where_src = offset_of(src) * blocks + lax.rem(src, blocks)
            if not first:
                where_src = jnp.maximum(where_src - blocks, 0)
            else:
                where_src = lax.rem(src, blocks)
            rel = perm_ref[p]
            qr = jnp.dot(att_ref[p], qt_ref[dst], preferred_element_type=jnp.float32)
            zero = jnp.zeros((size, block), jnp.bfloat16)
            sides = []
            for h in range(heads):
                scaled = qr[h * size : (h + 1) * size] * (prior_ref[rel * heads + h] * factor)
                parts = [zero] * heads
                parts[h] = scaled.astype(jnp.bfloat16)
                sides.append(jnp.concatenate(parts, axis=0))
            scores = jnp.dot(
                k_ref[where_src],
                jnp.concatenate(sides, axis=1),
                preferred_element_type=jnp.float32,
            )
            message = jnp.dot(
                msg_ref[p], vt_ref[where_src], preferred_element_type=jnp.float32
            ).astype(jnp.bfloat16)
            tile_words = bits_ref[slot] & valid
            edges = jnp.concatenate(
                [(tile_words[w : w + 1] & bit_of) != 0 for w in range(words)], axis=0
            )
            tile = []
            for h in range(heads):
                masked = jnp.where(edges, scores[:, h * block : (h + 1) * block], NEG)
                top = jnp.maximum(jnp.max(masked, axis=0, keepdims=True), FLOOR)
                weights = jnp.exp(masked - top)
                sums = jnp.sum(weights, axis=0, keepdims=True)
                out = jnp.dot(
                    message[h * size : (h + 1) * size],
                    weights.astype(jnp.bfloat16),
                    preferred_element_type=jnp.float32,
                )
                tile.append((top, sums, out))
            state.append((dst, tile))
        for dst, tile in state:
            for h, (top, sums, out) in enumerate(tile):
                m_old = ml_ref[dst, h : h + 1]
                l_old = ml_ref[dst, heads + h : heads + h + 1]
                m_new = jnp.maximum(m_old, top)
                keep = jnp.exp(m_old - m_new)
                take = jnp.exp(top - m_new)
                ml_ref[dst, h : h + 1] = m_new
                ml_ref[dst, heads + h : heads + h + 1] = l_old * keep + sums * take
                rows = pl.ds(h * size, size)
                acc_ref[dst, rows] = acc_ref[dst, rows] * keep + out * take
        return carry

    lax.fori_loop(0, (total + UNROLL - 1) // UNROLL, visit, 0)


def finish_kernel(n_rel, n_head, heads, ml_ref, acc_ref, types_ref, skip_ref, feat_ref, *refs):
    w_refs, refs = refs[:n_head], refs[n_head:]
    out_ref, acc_out, ml_out, acc_got, ml_got, hid_out, hid_got, rows_all, w_all, resid = refs[:10]
    part_send, part_recv, hid_send, hid_recv, row_send, row_recv, local = refs[10:]
    cols, block = acc_ref.shape[1], acc_ref.shape[2]
    size = cols // heads
    piece, width = resid.shape
    per = piece // block
    kinds = w_all.shape[1]
    r = lax.axis_index("rel")
    h = lax.axis_index("head")
    own_piece = h * n_rel + r

    fetches = [
        pltpu.make_async_copy(
            feat_ref.at[pl.ds(pl.multiple_of(own_piece * piece, piece), piece)], resid, local.at[n_head]
        )
    ]
    for t in range(n_head):
        fetches.append(pltpu.make_async_copy(w_refs[t], w_all.at[t], local.at[t]))
    for copy in fetches:
        copy.start()

    barrier = pltpu.get_barrier_semaphore()
    for t in range(1, n_rel):
        pl.semaphore_signal(barrier, inc=1, device_id={"rel": lax.rem(r + t, n_rel)})
    for t in range(1, n_head):
        pl.semaphore_signal(barrier, inc=1, device_id={"head": lax.rem(h + t, n_head)})
    for t in range(1, n_rel):
        dest = lax.rem(r + t, n_rel)
        for hh in range(n_head):
            for b in range(per):
                source = (hh * n_rel + dest) * per + b
                acc_out[t, hh * per + b] = acc_ref[source].astype(jnp.bfloat16)
                ml_out[t, hh * per + b] = ml_ref[source]
    pl.semaphore_wait(barrier, n_rel + n_head - 2)

    sends = []
    for t in range(1, n_rel):
        target = {"rel": lax.rem(r + t, n_rel)}
        for which, (src, dst) in enumerate(((ml_out, ml_got), (acc_out, acc_got))):
            sends.append(
                pltpu.make_async_remote_copy(
                    src_ref=src.at[t],
                    dst_ref=dst.at[t],
                    send_sem=part_send.at[which, t],
                    recv_sem=part_recv.at[which, t],
                    device_id=target,
                )
            )
    for copy in sends:
        copy.start()
    for copy in sends:
        copy.wait_recv()

    hid_sends = []
    for t in list(range(1, n_head)) + [0]:
        hh = lax.rem(h + t, n_head)
        for b in range(per):
            source = (hh * n_rel + r) * per + b
            place = hh * per + b
            tops = [ml_ref[source]] + [ml_got[s, place] for s in range(1, n_rel)]
            best = tops[0][:heads]
            for other in tops[1:]:
                best = jnp.maximum(best, other[:heads])
            scales = [jnp.exp(m[:heads] - best) for m in tops]
            total = sum(m[heads:] * scale for m, scale in zip(tops, scales))
            total = jnp.maximum(total, 1.0)
            sides = []
            for k in range(heads):
                rows = pl.ds(k * size, size)
                acc = acc_ref[source, rows] * scales[0][k : k + 1]
                for s in range(1, n_rel):
                    acc = acc + acc_got[s, place, rows].astype(jnp.float32) * scales[s][k : k + 1]
                sides.append(acc / total[k : k + 1])
            agg = jnp.concatenate(sides, axis=0)
            inner = math.sqrt(2.0 / math.pi) * (agg + 0.044715 * (agg * agg * agg))
            hidden = agg * (0.5 * (1.0 + jnp.tanh(inner)))
            target_ref = hid_out if t else hid_got
            target_ref[t, b * block : (b + 1) * block] = hidden.T.astype(jnp.bfloat16)
        if t:
            copy = pltpu.make_async_remote_copy(
                src_ref=hid_out.at[t],
                dst_ref=hid_got.at[t],
                send_sem=hid_send.at[t],
                recv_sem=hid_recv.at[t],
                device_id={"head": hh},
            )
            copy.start()
            hid_sends.append(copy)
    for copy in fetches:
        copy.wait()
    for copy in hid_sends:
        copy.wait_recv()

    for b in range(per):
        span = pl.ds(b * block, block)
        mask = column(types_ref[pl.ds(own_piece * per + b, 1), :])
        masks = [mask == float(kind) for kind in range(kinds)]
        hidden = jnp.concatenate([hid_got[t, span] for t in range(n_head)], axis=1)
        logit = jnp.full((block, block), skip_ref[0], jnp.float32)
        for kind in range(1, kinds):
            logit = jnp.where(masks[kind], skip_ref[kind], logit)
        gate = 1.0 / (1.0 + jnp.exp(-logit))
        wide = width // block
        total = None
        for kind in range(kinds):
            weights = jnp.concatenate([w_all[t, kind] for t in range(n_head)], axis=0)
            out = jnp.dot(hidden, weights, preferred_element_type=jnp.float32)
            pieces = [out[:, i * block : (i + 1) * block] for i in range(wide)]
            if total is None:
                total = pieces
            else:
                total = [jnp.where(masks[kind], n, o) for n, o in zip(pieces, total)]
        for i in range(wide):
            lanes = slice(i * block, (i + 1) * block)
            old = resid[span, lanes].astype(jnp.float32)
            done = (gate * total[i] + (1.0 - gate) * old).astype(jnp.bfloat16)
            rows_all[r, span, lanes] = done

    row_sends = []
    for t in range(1, n_rel):
        copy = pltpu.make_async_remote_copy(
            src_ref=rows_all.at[r],
            dst_ref=rows_all.at[r],
            send_sem=row_send.at[t],
            recv_sem=row_recv.at[t],
            device_id={"rel": lax.rem(r + t, n_rel)},
        )
        copy.start()
        row_sends.append(copy)
    for copy in row_sends:
        copy.wait_recv()
    for s in range(n_rel):
        out_ref[s * piece : (s + 1) * piece] = rows_all[s]
    for copy in sends + hid_sends + row_sends:
        copy.wait_send()


def per_device(
    features,
    node_type,
    w_query,
    w_key,
    w_value,
    rel_att,
    rel_msg,
    rel_prior,
    w_out,
    skip,
    rel_perm,
    tile_src,
    tile_dst,
    tile_bits,
    tile_count,
):
    node_rows, width = features.shape
    n_rel = lax.axis_size("rel")
    n_node = lax.axis_size("node")
    n_head = lax.axis_size("head")
    heads = rel_prior.shape[1]
    cols = w_query.shape[2]
    kinds = w_query.shape[0]
    head_size = cols // heads
    block = tile_bits.shape[2]
    words = tile_bits.shape[3]
    blocks = node_rows // block
    positions, tcap = tile_src.shape
    slots = positions * tcap
    factor = 1.0 / math.sqrt(head_size)
    steps = math.gcd(blocks // 2 if blocks % 2 == 0 else blocks, positions)
    per = blocks // steps
    per_pos = positions // steps
    types3 = node_type.reshape(steps, per, block)
    bf = jnp.bfloat16

    x_spec = pl.BlockSpec((per * block, width), lambda s, *_: (s, 0))
    t_spec = pl.BlockSpec((1, per, block), lambda s, *_: (s, 0, 0))
    w_spec = pl.BlockSpec((kinds, width, cols), lambda s, *_: (0, 0, 0))

    def tile_spec(count, rows, lanes):
        return pl.BlockSpec((count, rows, lanes), lambda s, *_: (s, 0, 0))

    keys, values_t = pl.pallas_call(
        kv_kernel,
        grid=(steps,),
        in_specs=[x_spec, t_spec, w_spec, w_spec],
        out_specs=[tile_spec(per, block, cols), tile_spec(per, cols, block)],
        out_shape=[
            jax.ShapeDtypeStruct((blocks, block, cols), bf),
            jax.ShapeDtypeStruct((blocks, cols, block), bf),
        ],
        name="project_kv",
    )(features, types3, w_key, w_value)

    far_k, far_v = [], []
    for shift in range(1, n_node):
        pairs = [(i, (i - shift) % n_node) for i in range(n_node)]
        far_k.append(lax.ppermute(keys, "node", pairs))
        far_v.append(lax.ppermute(values_t, "node", pairs))

    def rel_spec(i):
        return pl.BlockSpec(
            (1,) + rel_att.shape[1:], lambda s, perm: (perm[s * per_pos + i], 0, 0, 0)
        )

    rel_specs = [rel_spec(i) for i in range(per_pos)]
    query_t, att, msg = pl.pallas_call(
        functools.partial(q_kernel, per_pos),
        grid_spec=pltpu.PrefetchScalarGridSpec(
            num_scalar_prefetch=1,
            grid=(steps,),
            in_specs=[x_spec, t_spec, w_spec] + rel_specs * 2,
            out_specs=[
                tile_spec(per, cols, block),
                tile_spec(per_pos, cols, cols),
                tile_spec(per_pos, cols, cols),
            ],
        ),
        out_shape=[
            jax.ShapeDtypeStruct((blocks, cols, block), bf),
            jax.ShapeDtypeStruct((positions, cols, cols), bf),
            jax.ShapeDtypeStruct((positions, cols, cols), bf),
        ],
        name="project_q",
    )(rel_perm, features, types3, w_query, *([rel_att] * per_pos + [rel_msg] * per_pos))

    bits = tile_bits.transpose(0, 1, 3, 2).reshape(slots, words, block)
    scalars = (
        tile_count.reshape(positions),
        tile_src.reshape(slots),
        tile_dst.reshape(slots),
        rel_perm,
        rel_prior.reshape(-1),
    )
    smem = pl.BlockSpec(memory_space=pltpu.SMEM)
    vmem = pl.BlockSpec(memory_space=pltpu.VMEM)
    state = [
        jax.ShapeDtypeStruct((blocks, 2 * heads, block), jnp.float32),
        jax.ShapeDtypeStruct((blocks, cols, block), jnp.float32),
    ]

    def tiles(first, k_blocks, v_blocks, *carried):
        return pl.pallas_call(
            functools.partial(tile_kernel, first, n_node, heads, factor),
            in_specs=[smem] * 5 + [vmem] * (6 + len(carried)),
            out_specs=[vmem, vmem],
            out_shape=state,
            scratch_shapes=[pltpu.SMEM((slots + UNROLL,), jnp.int32)],
            compiler_params=pltpu.CompilerParams(vmem_limit_bytes=VMEM_BYTES),
            name="tiles_near" if first else "tiles_far",
        )(*scalars, query_t, k_blocks, v_blocks, bits, att, msg, *carried)

    ml, acc = tiles(True, keys, values_t)
    if n_node > 1:
        join = lambda arrs: arrs[0] if len(arrs) == 1 else jnp.concatenate(arrs, axis=0)
        ml, acc = tiles(False, join(far_k), join(far_v), ml, acc)

    gathered = [w_out]
    for shift in range(1, n_head):
        pairs = [(i, (i + shift) % n_head) for i in range(n_head)]
        gathered.append(lax.ppermute(w_out, "head", pairs))
    piece = node_rows // (n_rel * n_head)
    parts = n_head * piece // block
    dma = pltpu.SemaphoreType.DMA
    return pl.pallas_call(
        functools.partial(finish_kernel, n_rel, n_head, heads),
        in_specs=[vmem, vmem, vmem, smem] + [pl.BlockSpec(memory_space=pl.ANY)] * (1 + n_head),
        out_specs=vmem,
        out_shape=jax.ShapeDtypeStruct((n_rel * piece, width), bf),
        scratch_shapes=[
            pltpu.VMEM((n_rel, parts, cols, block), bf),
            pltpu.VMEM((n_rel, parts, 2 * heads, block), jnp.float32),
            pltpu.VMEM((n_rel, parts, cols, block), bf),
            pltpu.VMEM((n_rel, parts, 2 * heads, block), jnp.float32),
            pltpu.VMEM((n_head, piece, cols), bf),
            pltpu.VMEM((n_head, piece, cols), bf),
            pltpu.VMEM((n_rel, piece, width), bf),
            pltpu.VMEM((n_head,) + w_out.shape, bf),
            pltpu.VMEM((piece, width), bf),
            dma((2, n_rel)),
            dma((2, n_rel)),
            dma((n_head,)),
            dma((n_head,)),
            dma((n_rel,)),
            dma((n_rel,)),
            dma((n_head + 1,)),
        ],
        compiler_params=pltpu.CompilerParams(
            collective_id=0, has_side_effects=True, vmem_limit_bytes=VMEM_BYTES
        ),
        name="finish",
    )(ml, acc, node_type.reshape(blocks, block), skip, features, *gathered)


def solution(mesh):
    in_specs = (
        P("node", None),
        P("node"),
        P(None, None, "head"),
        P(None, None, "head"),
        P(None, None, "head"),
        P(None, "head", None, None),
        P(None, "head", None, None),
        P(None, "head"),
        P(None, "head", None),
        P(),
        P("rel"),
        P("rel", "node"),
        P("rel", "node"),
        P("rel", "node", None, None),
        P("rel", "node"),
    )
    out_specs = P(("node", "head"), None)
    return jax.shard_map(
        per_device, mesh=mesh, in_specs=in_specs, out_specs=out_specs, check_vma=False
    )
```

```python
import functools
import math

import jax
import jax.numpy as jnp
from jax import lax
from jax.experimental import pallas as pl
from jax.experimental.pallas import tpu as pltpu
from jax.sharding import PartitionSpec as P

NEG = -1e30
FLOOR = -1e29
UNROLL = 4
VMEM_BYTES = 28 * 1024 * 1024


def column(types_row):
    size = types_row.shape[1]
    return jnp.broadcast_to(types_row.astype(jnp.float32), (size, size)).T


def kv_kernel(x_ref, types_ref, wk_ref, wv_ref, k_ref, vt_ref):
    per, block, cols = k_ref.shape
    kinds = wk_ref.shape[0]
    x = x_ref[...]
    masks = [column(types_ref[0, b : b + 1, :]) for b in range(per)]
    totals = [None] * per
    for kind in range(kinds):
        both = jnp.concatenate([wk_ref[kind], wv_ref[kind]], axis=1)
        out = jnp.dot(x, both, preferred_element_type=jnp.float32)
        for b in range(per):
            piece = out[b * block : (b + 1) * block]
            pair = (piece[:, :cols], piece[:, cols:])
            if totals[b] is None:
                totals[b] = pair
            else:
                hit = masks[b] == float(kind)
                totals[b] = tuple(jnp.where(hit, n, o) for n, o in zip(pair, totals[b]))
    for b in range(per):
        k_ref[b] = totals[b][0].astype(jnp.bfloat16)
        vt_ref[b] = totals[b][1].T.astype(jnp.bfloat16)


def q_kernel(per_pos, perm_ref, x_ref, types_ref, wq_ref, *refs):
    att_refs, msg_refs = refs[:per_pos], refs[per_pos : 2 * per_pos]
    qt_ref, att_out, msg_out = refs[2 * per_pos :]
    per, block, cols = qt_ref.shape[0], qt_ref.shape[2], qt_ref.shape[1]
    kinds = wq_ref.shape[0]
    x = x_ref[...]
    wide = jnp.concatenate([wq_ref[kind] for kind in range(kinds)], axis=1)
    out = jnp.dot(x, wide, preferred_element_type=jnp.float32)
    for b in range(per):
        mask = column(types_ref[0, b : b + 1, :])
        piece = out[b * block : (b + 1) * block]
        total = piece[:, :cols]
        for kind in range(1, kinds):
            total = jnp.where(mask == float(kind), piece[:, kind * cols : (kind + 1) * cols], total)
        qt_ref[b] = total.T.astype(jnp.bfloat16)

    def diagonal(ref):
        heads, size = ref.shape[1], ref.shape[2]
        rows = []
        for h in range(heads):
            parts = [jnp.zeros((size, size), jnp.float32)] * heads
            parts[h] = ref[0, h].astype(jnp.float32)
            rows.append(jnp.concatenate(parts, axis=1))
        return jnp.concatenate(rows, axis=0)

    for i in range(per_pos):
        att_out[i] = diagonal(att_refs[i]).astype(jnp.bfloat16)
        msg_out[i] = diagonal(msg_refs[i]).T.astype(jnp.bfloat16)


def tile_kernel(
    first,
    n_node,
    heads,
    factor,
    count_ref,
    src_ref,
    dst_ref,
    perm_ref,
    prior_ref,
    qt_ref,
    k_ref,
    vt_ref,
    bits_ref,
    att_ref,
    msg_ref,
    *refs,
):
    if first:
        ml_ref, acc_ref, far_ref, list_ref = refs
    else:
        list_ref, ml_in, acc_in, ml_ref, acc_ref = refs
    positions = count_ref.shape[0]
    slots = src_ref.shape[0]
    tcap = slots // positions
    blocks = qt_ref.shape[0]
    cols, block = qt_ref.shape[1], qt_ref.shape[2]
    size = cols // heads
    words = bits_ref.shape[1]
    me = lax.axis_index("node")

    if first:
        ml_ref[:, :heads] = jnp.full((blocks, heads, block), FLOOR, jnp.float32)
        ml_ref[:, heads:] = jnp.zeros((blocks, heads, block), jnp.float32)
        acc_ref[...] = jnp.zeros_like(acc_ref)
    else:
        ml_ref[...] = ml_in[...]
        acc_ref[...] = acc_in[...]

    def offset_of(src):
        return lax.rem(src // blocks - me + n_node, n_node)

    if first:

        def gather_position(p, counts):
            near, far = counts
            count = count_ref[p]
            for k in range(tcap):
                slot = p * tcap + k
                list_ref[near] = slot
                far_ref[far] = slot
                live = jnp.where(k < count, 1, 0)
                local = jnp.where(offset_of(src_ref[slot]) == 0, live, 0)
                near = near + local
                far = far + (live - local)
            return near, far

        total, total_far = lax.fori_loop(0, positions, gather_position, (0, 0))
        for u in range(UNROLL):
            list_ref[total + u] = 0
            far_ref[total_far + u] = 0
        far_ref[slots + UNROLL] = total_far
    else:
        total = list_ref[slots + UNROLL]
    bit_of = lax.shift_left(
        jnp.int32(1), lax.broadcasted_iota(jnp.int32, (32, block), 0)
    )

    def visit(turn, carry):
        picks = []
        for u in range(UNROLL):
            index = turn * UNROLL + u
            slot = list_ref[index]
            valid = jnp.where(index < total, -1, 0)
            p = slot // tcap
            src = src_ref[slot]
            dst = dst_ref[slot]
            if first:
                source = lax.rem(src, blocks)
            else:
                source = (offset_of(src) - 1) * blocks + lax.rem(src, blocks)
                source = jnp.maximum(source, 0)
            picks.append((slot, valid, p, source, dst, perm_ref[p]))
        turned = [
            jnp.dot(att_ref[p], qt_ref[dst], preferred_element_type=jnp.float32)
            for _, _, p, _, dst, _ in picks
        ]
        messages = [
            jnp.dot(msg_ref[p], vt_ref[source], preferred_element_type=jnp.float32).astype(
                jnp.bfloat16
            )
            for _, _, p, source, _, _ in picks
        ]
        zero = jnp.zeros((size, block), jnp.bfloat16)
        scores = []
        for (_, _, _, source, _, rel), qr in zip(picks, turned):
            sides = []
            for h in range(heads):
                scaled = qr[h * size : (h + 1) * size] * (prior_ref[rel * heads + h] * factor)
                parts = [zero] * heads
                parts[h] = scaled.astype(jnp.bfloat16)
                sides.append(jnp.concatenate(parts, axis=0))
            scores.append(
                jnp.dot(
                    k_ref[source],
                    jnp.concatenate(sides, axis=1),
                    preferred_element_type=jnp.float32,
                )
            )
        softened = []
        for (slot, valid, _, _, _, _), score in zip(picks, scores):
            tile_words = bits_ref[slot] & valid
            edges = jnp.concatenate(
                [(tile_words[w : w + 1] & bit_of) != 0 for w in range(words)], axis=0
            )
            for h in range(heads):
                masked = jnp.where(edges, score[:, h * block : (h + 1) * block], NEG)
                top = jnp.maximum(jnp.max(masked, axis=0, keepdims=True), FLOOR)
                weights = jnp.exp(masked - top)
                sums = jnp.sum(weights, axis=0, keepdims=True)
                softened.append((top, sums, weights.astype(jnp.bfloat16)))
        state = []
        for u, (_, _, _, _, dst, _) in enumerate(picks):
            tile = []
            for h in range(heads):
                top, sums, weights = softened[u * heads + h]
                out = jnp.dot(
                    messages[u][h * size : (h + 1) * size],
                    weights,
                    preferred_element_type=jnp.float32,
                )
                tile.append((top, sums, out))
            state.append((dst, tile))
        for dst, tile in state:
            for h, (top, sums, out) in enumerate(tile):
                m_old = ml_ref[dst, h : h + 1]
                l_old = ml_ref[dst, heads + h : heads + h + 1]
                m_new = jnp.maximum(m_old, top)
                keep = jnp.exp(m_old - m_new)
                take = jnp.exp(top - m_new)
                ml_ref[dst, h : h + 1] = m_new
                ml_ref[dst, heads + h : heads + h + 1] = l_old * keep + sums * take
                rows = pl.ds(h * size, size)
                acc_ref[dst, rows] = acc_ref[dst, rows] * keep + out * take
        return carry

    lax.fori_loop(0, (total + UNROLL - 1) // UNROLL, visit, 0)


def finish_kernel(n_rel, n_head, heads, ml_ref, acc_ref, types_ref, skip_ref, feat_ref, *refs):
    w_refs, refs = refs[:n_head], refs[n_head:]
    out_ref, acc_out, ml_out, acc_got, ml_got, hid_out, hid_got, rows_all, w_all, resid = refs[:10]
    part_send, part_recv, hid_send, hid_recv, row_send, row_recv, local = refs[10:]
    cols, block = acc_ref.shape[1], acc_ref.shape[2]
    size = cols // heads
    piece, width = resid.shape
    per = piece // block
    kinds = w_all.shape[1]
    r = lax.axis_index("rel")
    h = lax.axis_index("head")
    own_piece = h * n_rel + r

    fetches = [
        pltpu.make_async_copy(
            feat_ref.at[pl.ds(pl.multiple_of(own_piece * piece, piece), piece)], resid, local.at[n_head]
        )
    ]
    for t in range(n_head):
        fetches.append(pltpu.make_async_copy(w_refs[t], w_all.at[t], local.at[t]))
    for copy in fetches:
        copy.start()

    barrier = pltpu.get_barrier_semaphore()
    for t in range(1, n_rel):
        pl.semaphore_signal(barrier, inc=1, device_id={"rel": lax.rem(r + t, n_rel)})
    for t in range(1, n_head):
        pl.semaphore_signal(barrier, inc=1, device_id={"head": lax.rem(h + t, n_head)})
    for t in range(1, n_rel):
        dest = lax.rem(r + t, n_rel)
        for hh in range(n_head):
            for b in range(per):
                source = (hh * n_rel + dest) * per + b
                acc_out[t, hh * per + b] = acc_ref[source].astype(jnp.bfloat16)
                ml_out[t, hh * per + b] = ml_ref[source]
    pl.semaphore_wait(barrier, n_rel + n_head - 2)

    sends = []
    for t in range(1, n_rel):
        target = {"rel": lax.rem(r + t, n_rel)}
        for which, (src, dst) in enumerate(((ml_out, ml_got), (acc_out, acc_got))):
            sends.append(
                pltpu.make_async_remote_copy(
                    src_ref=src.at[t],
                    dst_ref=dst.at[t],
                    send_sem=part_send.at[which, t],
                    recv_sem=part_recv.at[which, t],
                    device_id=target,
                )
            )
    for copy in sends:
        copy.start()
    for copy in sends:
        copy.wait_recv()

    hid_sends = []
    for t in list(range(1, n_head)) + [0]:
        hh = lax.rem(h + t, n_head)
        for b in range(per):
            source = (hh * n_rel + r) * per + b
            place = hh * per + b
            tops = [ml_ref[source]] + [ml_got[s, place] for s in range(1, n_rel)]
            best = tops[0][:heads]
            for other in tops[1:]:
                best = jnp.maximum(best, other[:heads])
            scales = [jnp.exp(m[:heads] - best) for m in tops]
            total = sum(m[heads:] * scale for m, scale in zip(tops, scales))
            total = jnp.maximum(total, 1.0)
            sides = []
            for k in range(heads):
                rows = pl.ds(k * size, size)
                acc = acc_ref[source, rows] * scales[0][k : k + 1]
                for s in range(1, n_rel):
                    acc = acc + acc_got[s, place, rows].astype(jnp.float32) * scales[s][k : k + 1]
                sides.append(acc / total[k : k + 1])
            agg = jnp.concatenate(sides, axis=0)
            inner = math.sqrt(2.0 / math.pi) * (agg + 0.044715 * (agg * agg * agg))
            hidden = agg * (0.5 * (1.0 + jnp.tanh(inner)))
            target_ref = hid_out if t else hid_got
            target_ref[t, b * block : (b + 1) * block] = hidden.T.astype(jnp.bfloat16)
        if t:
            copy = pltpu.make_async_remote_copy(
                src_ref=hid_out.at[t],
                dst_ref=hid_got.at[t],
                send_sem=hid_send.at[t],
                recv_sem=hid_recv.at[t],
                device_id={"head": hh},
            )
            copy.start()
            hid_sends.append(copy)
    for copy in fetches:
        copy.wait()
    for copy in hid_sends:
        copy.wait_recv()

    for b in range(per):
        span = pl.ds(b * block, block)
        mask = column(types_ref[pl.ds(own_piece * per + b, 1), :])
        masks = [mask == float(kind) for kind in range(kinds)]
        hidden = jnp.concatenate([hid_got[t, span] for t in range(n_head)], axis=1)
        logit = jnp.full((block, block), skip_ref[0], jnp.float32)
        for kind in range(1, kinds):
            logit = jnp.where(masks[kind], skip_ref[kind], logit)
        gate = 1.0 / (1.0 + jnp.exp(-logit))
        wide = width // block
        total = None
        for kind in range(kinds):
            weights = jnp.concatenate([w_all[t, kind] for t in range(n_head)], axis=0)
            out = jnp.dot(hidden, weights, preferred_element_type=jnp.float32)
            pieces = [out[:, i * block : (i + 1) * block] for i in range(wide)]
            if total is None:
                total = pieces
            else:
                total = [jnp.where(masks[kind], n, o) for n, o in zip(pieces, total)]
        for i in range(wide):
            lanes = slice(i * block, (i + 1) * block)
            old = resid[span, lanes].astype(jnp.float32)
            done = (gate * total[i] + (1.0 - gate) * old).astype(jnp.bfloat16)
            rows_all[r, span, lanes] = done

    row_sends = []
    for t in range(1, n_rel):
        copy = pltpu.make_async_remote_copy(
            src_ref=rows_all.at[r],
            dst_ref=rows_all.at[r],
            send_sem=row_send.at[t],
            recv_sem=row_recv.at[t],
            device_id={"rel": lax.rem(r + t, n_rel)},
        )
        copy.start()
        row_sends.append(copy)
    for copy in row_sends:
        copy.wait_recv()
    for s in range(n_rel):
        out_ref[s * piece : (s + 1) * piece] = rows_all[s]
    for copy in sends + hid_sends + row_sends:
        copy.wait_send()


def per_device(
    features,
    node_type,
    w_query,
    w_key,
    w_value,
    rel_att,
    rel_msg,
    rel_prior,
    w_out,
    skip,
    rel_perm,
    tile_src,
    tile_dst,
    tile_bits,
    tile_count,
):
    node_rows, width = features.shape
    n_rel = lax.axis_size("rel")
    n_node = lax.axis_size("node")
    n_head = lax.axis_size("head")
    heads = rel_prior.shape[1]
    cols = w_query.shape[2]
    kinds = w_query.shape[0]
    head_size = cols // heads
    block = tile_bits.shape[2]
    words = tile_bits.shape[3]
    blocks = node_rows // block
    positions, tcap = tile_src.shape
    slots = positions * tcap
    factor = 1.0 / math.sqrt(head_size)
    steps = math.gcd(blocks // 4 if blocks % 4 == 0 else blocks, positions)
    per = blocks // steps
    per_pos = positions // steps
    types3 = node_type.reshape(steps, per, block)
    bf = jnp.bfloat16

    x_spec = pl.BlockSpec((per * block, width), lambda s, *_: (s, 0))
    t_spec = pl.BlockSpec((1, per, block), lambda s, *_: (s, 0, 0))
    w_spec = pl.BlockSpec((kinds, width, cols), lambda s, *_: (0, 0, 0))

    def tile_spec(count, rows, lanes):
        return pl.BlockSpec((count, rows, lanes), lambda s, *_: (s, 0, 0))

    keys, values_t = pl.pallas_call(
        kv_kernel,
        grid=(steps,),
        in_specs=[x_spec, t_spec, w_spec, w_spec],
        out_specs=[tile_spec(per, block, cols), tile_spec(per, cols, block)],
        out_shape=[
            jax.ShapeDtypeStruct((blocks, block, cols), bf),
            jax.ShapeDtypeStruct((blocks, cols, block), bf),
        ],
        name="project_kv",
    )(features, types3, w_key, w_value)

    far_k, far_v = [], []
    for shift in range(1, n_node):
        pairs = [(i, (i - shift) % n_node) for i in range(n_node)]
        far_k.append(lax.ppermute(keys, "node", pairs))
        far_v.append(lax.ppermute(values_t, "node", pairs))

    def rel_spec(i):
        return pl.BlockSpec(
            (1,) + rel_att.shape[1:], lambda s, perm: (perm[s * per_pos + i], 0, 0, 0)
        )

    rel_specs = [rel_spec(i) for i in range(per_pos)]
    query_t, att, msg = pl.pallas_call(
        functools.partial(q_kernel, per_pos),
        grid_spec=pltpu.PrefetchScalarGridSpec(
            num_scalar_prefetch=1,
            grid=(steps,),
            in_specs=[x_spec, t_spec, w_spec] + rel_specs * 2,
            out_specs=[
                tile_spec(per, cols, block),
                tile_spec(per_pos, cols, cols),
                tile_spec(per_pos, cols, cols),
            ],
        ),
        out_shape=[
            jax.ShapeDtypeStruct((blocks, cols, block), bf),
            jax.ShapeDtypeStruct((positions, cols, cols), bf),
            jax.ShapeDtypeStruct((positions, cols, cols), bf),
        ],
        name="project_q",
    )(rel_perm, features, types3, w_query, *([rel_att] * per_pos + [rel_msg] * per_pos))

    bits = tile_bits.transpose(0, 1, 3, 2).reshape(slots, words, block)
    scalars = (
        tile_count.reshape(positions),
        tile_src.reshape(slots),
        tile_dst.reshape(slots),
        rel_perm,
        rel_prior.reshape(-1),
    )
    smem = pl.BlockSpec(memory_space=pltpu.SMEM)
    vmem = pl.BlockSpec(memory_space=pltpu.VMEM)
    state = [
        jax.ShapeDtypeStruct((blocks, 2 * heads, block), jnp.float32),
        jax.ShapeDtypeStruct((blocks, cols, block), jnp.float32),
    ]

    listed = jax.ShapeDtypeStruct((slots + UNROLL + 1,), jnp.int32)

    def tiles(first, k_blocks, v_blocks, order=(), carried=()):
        return pl.pallas_call(
            functools.partial(tile_kernel, first, n_node, heads, factor),
            in_specs=[smem] * 5 + [vmem] * 6 + [smem] * len(order) + [vmem] * len(carried),
            out_specs=[vmem, vmem] + [smem] * first,
            out_shape=state + [listed] * first,
            scratch_shapes=[pltpu.SMEM(listed.shape, jnp.int32)] * first,
            compiler_params=pltpu.CompilerParams(vmem_limit_bytes=VMEM_BYTES),
            name="tiles_near" if first else "tiles_far",
        )(*scalars, query_t, k_blocks, v_blocks, bits, att, msg, *order, *carried)

    ml, acc, far_list = tiles(True, keys, values_t)
    if n_node > 1:
        join = lambda arrs: arrs[0] if len(arrs) == 1 else jnp.concatenate(arrs, axis=0)
        ml, acc = tiles(False, join(far_k), join(far_v), (far_list,), (ml, acc))

    gathered = [w_out]
    for shift in range(1, n_head):
        pairs = [(i, (i + shift) % n_head) for i in range(n_head)]
        gathered.append(lax.ppermute(w_out, "head", pairs))
    piece = node_rows // (n_rel * n_head)
    parts = n_head * piece // block
    dma = pltpu.SemaphoreType.DMA
    return pl.pallas_call(
        functools.partial(finish_kernel, n_rel, n_head, heads),
        in_specs=[vmem, vmem, vmem, smem] + [pl.BlockSpec(memory_space=pl.ANY)] * (1 + n_head),
        out_specs=vmem,
        out_shape=jax.ShapeDtypeStruct((n_rel * piece, width), bf),
        scratch_shapes=[
            pltpu.VMEM((n_rel, parts, cols, block), bf),
            pltpu.VMEM((n_rel, parts, 2 * heads, block), jnp.float32),
            pltpu.VMEM((n_rel, parts, cols, block), bf),
            pltpu.VMEM((n_rel, parts, 2 * heads, block), jnp.float32),
            pltpu.VMEM((n_head, piece, cols), bf),
            pltpu.VMEM((n_head, piece, cols), bf),
            pltpu.VMEM((n_rel, piece, width), bf),
            pltpu.VMEM((n_head,) + w_out.shape, bf),
            pltpu.VMEM((piece, width), bf),
            dma((2, n_rel)),
            dma((2, n_rel)),
            dma((n_head,)),
            dma((n_head,)),
            dma((n_rel,)),
            dma((n_rel,)),
            dma((n_head + 1,)),
        ],
        compiler_params=pltpu.CompilerParams(
            collective_id=0, has_side_effects=True, vmem_limit_bytes=VMEM_BYTES
        ),
        name="finish",
    )(ml, acc, node_type.reshape(blocks, block), skip, features, *gathered)


def solution(mesh):
    in_specs = (
        P("node", None),
        P("node"),
        P(None, None, "head"),
        P(None, None, "head"),
        P(None, None, "head"),
        P(None, "head", None, None),
        P(None, "head", None, None),
        P(None, "head"),
        P(None, "head", None),
        P(),
        P("rel"),
        P("rel", "node"),
        P("rel", "node"),
        P("rel", "node", None, None),
        P("rel", "node"),
    )
    out_specs = P(("node", "head"), None)
    return jax.shard_map(
        per_device, mesh=mesh, in_specs=in_specs, out_specs=out_specs, check_vma=False
    )
```
